32 devices in a mesh: gx: 4 (over z), gy: 2 (over y), gz: 4 (over x, core).
Axes of the slice: x: 2, y: 2, z: 4, core: 2. Of those that a mesh axis runs over, the one named last changes fastest.
Arguments:
- colloc: bfloat16 [768, 4000], P(('gx', 'gy')), may hold values from -6 to 6
- occ_coeffs: bfloat16 [4000, 1024], P(None, 'gz'), may hold values from -0.09375 to 0.09375
- core: bfloat16 [768, 2, 384], P('gx', 'gy'), may hold values from -6.246567e-05 to 6.246567e-05
Outputs:
- coulomb: float32 [96, 4000], P(('gx', 'gz'), 'gy')
- exchange: float32 [96, 4000], P(('gx', 'gz'), 'gy')
The draws below stay inside these ranges and needn't reach their ends.
All inputs are finite; a program needn't handle non-finite values.
Results may differ from the reference program's by a relative error of at most 0.0089.
Values may be sent and summed in bfloat16 or wider, within the bound.
A program may use at most 64 MiB of HBM per device.

```python
import jax
import jax.numpy as jnp
from jax import lax

N = 4000
O = 1024
PB = 96
W = 96
P_SIZE = 768
N_GX = 4
N_GY = 2
N_GZ = 4


def block_levels(rng, extent, cuts, least, top_value):
    def one(position, blocks):
        heights = jax.random.uniform(jax.random.fold_in(jax.random.fold_in(rng, 6), position), (blocks,), jnp.float32, least / len(cuts), top_value / len(cuts))
        return jnp.repeat(jnp.exp(heights), extent[position] // blocks).reshape((-1,) + (1,) * (len(extent) - position - 1))

    loudness = one(*cuts[0])
    for cut in cuts[1:]:
        loudness = loudness * one(*cut)
    return loudness


def scatter_about(stream_key, extent, deviation, reach, pieces=(), kind=jnp.bfloat16):
    values = deviation * jax.random.normal(stream_key, extent, jnp.float32)
    if pieces:
        values = values * block_levels(stream_key, extent, pieces, -0.22, 0.18)
    return jnp.clip(values, -reach, reach).astype(kind)


def setup_inputs(seed: int = 0) -> dict:
    splits = jax.random.split(jax.random.key(seed), 4)
    colloc = scatter_about(splits[0], (P_SIZE, N), 1.0, 6.0, ((0, 8),))
    occ_coeffs = scatter_about(splits[1], (N, O), N ** -0.5, 0.09375, ((1, 4),))
    core = scatter_about(splits[2], (P_SIZE, N_GY, N_GX * PB), (0.008 / (PB * N_GX * N_GY)), 6.246566772460938e-05, ((0, 4), (1, 2)))
    return dict(colloc=colloc, occ_coeffs=occ_coeffs, core=core)


def reference(colloc, occ_coeffs, core):
    zmat = core.reshape(P_SIZE, N_GY, N_GX, PB).transpose(0, 2, 1, 3).reshape(P_SIZE, P_SIZE)
    occ = jnp.dot(colloc, occ_coeffs, preferred_element_type=jnp.float32).astype(jnp.bfloat16)
    density = jnp.sum(jnp.square(occ.astype(jnp.float32)), axis=1).astype(jnp.bfloat16)
    potential = jnp.dot(zmat, density, preferred_element_type=jnp.float32)
    window = colloc[:, :W]
    block_rows = PB * N_GY
    quarter = O // N_GZ

    def add_block(index, acc):
        start = (index * block_rows).astype(jnp.int32)
        occ_rows = lax.dynamic_slice_in_dim(occ, start, block_rows, 0)
        core_rows = lax.dynamic_slice_in_dim(zmat, start, block_rows, 0)
        win_rows = lax.dynamic_slice_in_dim(window, start, block_rows, 0)
        for group in range(N_GZ):
            left = occ_rows[:, group * quarter:(group + 1) * quarter]
            right = occ[:, group * quarter:(group + 1) * quarter]
            gram = jnp.dot(left, right.T, preferred_element_type=jnp.float32)
            mixed = (core_rows.astype(jnp.float32) * gram).astype(jnp.bfloat16)
            acc = acc + jnp.dot(mixed.T, win_rows, preferred_element_type=jnp.float32)
        return acc

    totals = lax.fori_loop(0, N_GX, add_block, jnp.zeros((P_SIZE, W), jnp.float32))
    weighted = (window.astype(jnp.float32) * potential[:, None]).astype(jnp.bfloat16)
    coulomb = jnp.dot(weighted.T, colloc, preferred_element_type=jnp.float32)
    exchange = jnp.dot(totals.astype(jnp.bfloat16).T, colloc, preferred_element_type=jnp.float32)
    return (coulomb, exchange)
```

```python
import functools

import jax
import jax.numpy as jnp
import numpy as np
from jax import lax
from jax.experimental import pallas as pl
from jax.experimental.pallas import tpu as pltpu
from jax.sharding import PartitionSpec as P

W = 96
LANES = 128
DEPTH = 1024
MESH = pl.DeviceIdType.MESH
F32 = jnp.float32
BF16 = jnp.bfloat16


def up(value, step):
    return -(-value // step) * step


def dot(left, right, left_dim, right_dim):
    return lax.dot_general(
        left, right, (((left_dim,), (right_dim,)), ((), ())), preferred_element_type=F32
    )


def kernel(
    dims,
    colloc_hbm,
    coeffs_hbm,
    core_hbm,
    place_hbm,
    coul_ref,
    exch_ref,
    vals,
    coeffs,
    core,
    place,
    col_occ,
    row_occ,
    wins,
    win_t,
    parts,
    pot_send,
    pot_recv,
    tot_send,
    tot_recv,
    y_send,
    y_recv,
    z_send,
    z_recv,
    load_sem,
    depth_sem,
    col_sem,
    row_sem,
    win_sem,
    pot_sem,
    tot_sem,
    y_sem,
    z_sem,
):
    gx_size, gy_size, gz_size, rows, pad_rows, width, piece = dims
    gx, gy, gz = lax.axis_index("gx"), lax.axis_index("gy"), lax.axis_index("gz")
    points, total = vals.shape
    band = gx_size * pad_rows
    pieces = parts.shape[1]

    def turn(pos, step, size):
        return lax.rem(pos + step, size) if step else pos

    def peer(dx, dy, dz):
        return (turn(gx, dx, gx_size), turn(gy, dy, gy_size), turn(gz, dz, gz_size))

    loads = [
        pltpu.make_async_copy(colloc_hbm, vals, load_sem.at[0]),
        pltpu.make_async_copy(core_hbm, core, load_sem.at[1]),
        pltpu.make_async_copy(place_hbm, place, load_sem.at[2]),
    ]
    spans = [(s, min(DEPTH, total - s)) for s in range(0, total, DEPTH)]
    depth_loads = [
        pltpu.make_async_copy(
            coeffs_hbm.at[pl.ds(s, n)], coeffs.at[pl.ds(s, n)], depth_sem.at[i]
        )
        for i, (s, n) in enumerate(spans)
    ]
    loads[0].start()
    for load in depth_loads:
        load.start()
    loads[1].start()
    loads[2].start()

    barrier = pltpu.get_barrier_semaphore()
    mates = [(dx, 0, dz) for dx in range(gx_size) for dz in range(gz_size) if dx or dz]
    mates += [(0, dy, dz) for dy in range(1, gy_size) for dz in range(gz_size)]
    for mate in mates:
        pl.semaphore_signal(barrier, inc=1, device_id=peer(*mate), device_id_type=MESH)

    sent = []

    def send(src, dst, sems, out_slot, in_slot, target):
        copy = pltpu.make_async_remote_copy(
            src_ref=src,
            dst_ref=dst,
            send_sem=sems.at[(0,) + out_slot],
            recv_sem=sems.at[(1,) + in_slot],
            device_id=target,
            device_id_type=MESH,
        )
        copy.start()
        sent.append(copy)

    def arrive(dst, sems, in_slot, source):
        pltpu.make_async_remote_copy(
            src_ref=dst,
            dst_ref=dst,
            send_sem=sems.at[(0,) + in_slot],
            recv_sem=sems.at[(1,) + in_slot],
            device_id=source,
            device_id_type=MESH,
        ).wait_recv()

    loads[0].wait()
    occ = jnp.zeros((points, coeffs.shape[1]), F32)
    for load, (s, n) in zip(depth_loads, spans):
        load.wait()
        occ += dot(vals[:, s : s + n], coeffs[s : s + n, :], 1, 0)
    occ = occ.astype(BF16)
    col_occ[gx] = occ
    row_occ[gy] = occ
    pl.semaphore_wait(barrier, len(mates))
    for dx in range(1, gx_size):
        send(col_occ.at[gx], col_occ.at[gx], col_sem, (dx,), (gx,), peer(dx, 0, 0))
    for dy in range(1, gy_size):
        send(row_occ.at[gy], row_occ.at[gy], row_sem, (dy,), (gy,), peer(0, dy, 0))
    window = vals.at[:, pl.ds(0, wins.shape[2])]
    for dy in range(1, gy_size):
        send(window, wins.at[gy], win_sem, (dy,), (gy,), peer(0, dy, 0))

    loads[1].wait()
    loads[2].wait()
    own_win = vals[:, : wins.shape[2]]
    wins[gy] = own_win
    spread = place[...]
    win_t[...] = dot(spread, own_win, 0, 1).reshape(gz_size, band, points)
    for h in range(gy_size):
        for c in range(pieces):
            s = h * width + c * piece
            n = min(piece, width - c * piece)
            parts[h, c, :, :n] = vals[:, s : s + n]
            if n < piece:
                parts[h, c, :, n:] = jnp.zeros((points, piece - n), BF16)

    for dy in range(1, gy_size):
        slot = turn(gy, dy, gy_size)
        arrive(wins.at[slot], win_sem, (slot,), peer(0, dy, 0))
    win_rows = dot(wins[...].reshape(gy_size * points, -1), spread, 1, 0).astype(BF16)
    for dx in range(1, gx_size):
        slot = turn(gx, dx, gx_size)
        arrive(col_occ.at[slot], col_sem, (slot,), peer(dx, 0, 0))
    cols = col_occ[...].reshape(gx_size * points, -1)
    square = jnp.square(cols.astype(F32))
    high = square.astype(BF16)
    low = (square - high.astype(F32)).astype(BF16)
    ones = jnp.ones((8, square.shape[1]), BF16)
    density = dot(ones, high, 1, 1) + dot(ones, low, 1, 1)
    core_vals = core[...]
    potential = dot(density.astype(BF16), core_vals, 1, 1)
    for h in range(gy_size):
        pot_send[h] = potential[:, h * points : (h + 1) * points]
    mine = gy * gz_size + gz
    for dy in range(gy_size):
        for dz in range(gz_size):
            if dy or dz:
                src = pot_send.at[turn(gy, dy, gy_size)]
                out = (dy * gz_size + dz,)
                send(src, pot_recv.at[mine], pot_sem, out, (mine,), peer(0, dy, dz))

    for dy in range(1, gy_size):
        slot = turn(gy, dy, gy_size)
        arrive(row_occ.at[slot], row_sem, (slot,), peer(0, dy, 0))
    gram = dot(row_occ[...].reshape(gy_size * points, -1), cols, 1, 1)
    mixed = (core_vals.astype(F32) * gram).astype(BF16)
    totals = dot(win_rows, mixed, 0, 0)
    for a in range(gx_size):
        block = totals[:, a * points : (a + 1) * points].astype(BF16)
        tot_send[a] = block.reshape(gz_size, band, points)
    home = gx * gz_size + gz
    for dx in range(gx_size):
        for dz in range(gz_size):
            if dx or dz:
                to = peer(dx, 0, dz)
                src = tot_send.at[to[0], to[2]]
                out = (dx * gz_size + dz,)
                send(src, tot_recv.at[home], tot_sem, out, (home,), to)

    def spread_out(index, left):
        kept = []
        for c in range(pieces):
            for dy in range(1, gy_size):
                h = turn(gy, dy, gy_size)
                y_send[index, c, h] = dot(left, parts[h, c], 1, 0).astype(BF16)
                slots = (index, c, dy), (index, c, gy)
                dst = y_recv.at[index, c, gy]
                send(y_send.at[index, c, h], dst, y_sem, *slots, peer(0, dy, 0))
        for c in range(pieces):
            kept.append(dot(left, parts[gy, c], 1, 0))
        return kept

    pot = pot_send[gy]
    for dy in range(gy_size):
        for dz in range(gz_size):
            if dy or dz:
                to = peer(0, dy, dz)
                slot = to[1] * gz_size + to[2]
                arrive(pot_recv.at[slot], pot_sem, (slot,), to)
                pot += pot_recv[slot]
    coul_kept = spread_out(0, (win_t[gz] * pot[:1]).astype(BF16))

    owned = tot_send[gx, gz].astype(F32)
    for dx in range(gx_size):
        for dz in range(gz_size):
            if dx or dz:
                to = peer(dx, 0, dz)
                slot = to[0] * gz_size + to[2]
                arrive(tot_recv.at[slot], tot_sem, (slot,), to)
                owned += tot_recv[slot].astype(F32)
    exch_kept = spread_out(1, owned.astype(BF16))

    for index, kept in enumerate((coul_kept, exch_kept)):
        for c in range(pieces):
            acc = kept[c]
            for dy in range(1, gy_size):
                slot = turn(gy, dy, gy_size)
                dst = y_recv.at[index, c, slot]
                arrive(dst, y_sem, (index, c, slot), peer(0, dy, 0))
                acc += y_recv[index, c, slot].astype(F32)
            z_send[index, c] = acc.reshape(gx_size, pad_rows, piece).astype(BF16)
            for dx in range(1, gx_size):
                a = turn(gx, dx, gx_size)
                slots = (index, c, dx), (index, c, gx)
                dst = z_recv.at[index, c, gx]
                send(z_send.at[index, c, a], dst, z_sem, *slots, peer(dx, 0, 0))

    for index, out_ref in enumerate((coul_ref, exch_ref)):
        for c in range(pieces):
            acc = z_send[index, c, gx].astype(F32)
            for dx in range(1, gx_size):
                slot = turn(gx, dx, gx_size)
                dst = z_recv.at[index, c, slot]
                arrive(dst, z_sem, (index, c, slot), peer(dx, 0, 0))
                acc += z_recv[index, c, slot].astype(F32)
            n = min(piece, width - c * piece)
            out_ref[:, c * piece : c * piece + n] = acc[:rows, :n]

    for copy in sent:
        copy.wait_send()


def local(colloc, occ_coeffs, core):
    points, total = colloc.shape
    gx_size = lax.axis_size("gx")
    gy_size = lax.axis_size("gy")
    gz_size = lax.axis_size("gz")
    occupied = occ_coeffs.shape[1]
    rows = W // (gx_size * gz_size)
    pad_rows = up(rows, 8)
    width = total // gy_size
    piece = min(512, up(width, LANES))
    pieces = -(-width // piece)
    row_count, flat = core.shape[0], core.shape[2]
    band = gx_size * pad_rows
    lanes = up(W, LANES)

    place = np.zeros((lanes, gz_size, gx_size, pad_rows), np.float32)
    for a in range(gx_size):
        for g in range(gz_size):
            for k in range(rows):
                place[(a * gz_size + g) * rows + k, g, a, k] = 1
    place = jnp.asarray(place.reshape(lanes, gz_size * band), BF16)

    dims = (gx_size, gy_size, gz_size, rows, pad_rows, width, piece)
    dma = pltpu.SemaphoreType.DMA
    vmem = pltpu.VMEM
    out = jax.ShapeDtypeStruct((rows, width), F32)
    return pl.pallas_call(
        functools.partial(kernel, dims),
        out_shape=(out, out),
        in_specs=[pl.BlockSpec(memory_space=pltpu.HBM)] * 4,
        out_specs=(pl.BlockSpec(memory_space=pltpu.VMEM),) * 2,
        scratch_shapes=[
            vmem((points, total), BF16),
            vmem((total, occupied), BF16),
            vmem((row_count, flat), BF16),
            vmem((lanes, gz_size * band), BF16),
            vmem((gx_size, points, occupied), BF16),
            vmem((gy_size, points, occupied), BF16),
            vmem((gy_size, points, lanes), BF16),
            vmem((gz_size, band, points), F32),
            vmem((gy_size, pieces, points, piece), BF16),
            vmem((gy_size, 8, points), F32),
            vmem((gy_size * gz_size, 8, points), F32),
            vmem((gx_size, gz_size, band, points), BF16),
            vmem((gx_size * gz_size, band, points), BF16),
            vmem((2, pieces, gy_size, band, piece), BF16),
            vmem((2, pieces, gy_size, band, piece), BF16),
            vmem((2, pieces, gx_size, pad_rows, piece), BF16),
            vmem((2, pieces, gx_size, pad_rows, piece), BF16),
            dma((3,)),
            dma((-(-total // DEPTH),)),
            dma((2, gx_size)),
            dma((2, gy_size)),
            dma((2, gy_size)),
            dma((2, gy_size * gz_size)),
            dma((2, gx_size * gz_size)),
            dma((2, 2, pieces, gy_size)),
            dma((2, 2, pieces, gx_size)),
        ],
        compiler_params=pltpu.CompilerParams(
            collective_id=0, has_side_effects=True, vmem_limit_bytes=48 * 1024 * 1024
        ),
    )(colloc, occ_coeffs, core.reshape(row_count, flat), place)


def solution(mesh):
    in_specs = (P(("gx", "gy"), None), P(None, "gz"), P("gx", "gy", None))
    out_specs = (P(("gx", "gz"), "gy"), P(("gx", "gz"), "gy"))
    return jax.shard_map(local, mesh=mesh, in_specs=in_specs, out_specs=out_specs, check_vma=False)
```

```python
import functools

import jax
import jax.numpy as jnp
import numpy as np
from jax import lax
from jax.experimental import pallas as pl
from jax.experimental.pallas import tpu as pltpu
from jax.sharding import PartitionSpec as P

W = 96
LANES = 128
DEPTH = 1024
MESH = pl.DeviceIdType.MESH
F32 = jnp.float32
BF16 = jnp.bfloat16


def up(value, step):
    return -(-value // step) * step


def dot(left, right, left_dim, right_dim):
    return lax.dot_general(
        left, right, (((left_dim,), (right_dim,)), ((), ())), preferred_element_type=F32
    )


def kernel(
    dims,
    colloc_hbm,
    coeffs_hbm,
    core_hbm,
    place_hbm,
    fold_hbm,
    out_ref,
    vals,
    coeffs,
    core,
    place,
    fold,
    cores,
    col_occ,
    row_occ,
    wins,
    win_t,
    parts,
    pot_send,
    pot_recv,
    tot_send,
    tot_recv,
    y_send,
    y_recv,
    z_send,
    z_recv,
    load_sem,
    depth_sem,
    col_sem,
    row_sem,
    win_sem,
    pot_sem,
    tot_sem,
    y_sem,
    z_sem,
):
    gx_size, gy_size, gz_size, rows, pad_rows, width, piece, tails = dims
    gx, gy, gz = lax.axis_index("gx"), lax.axis_index("gy"), lax.axis_index("gz")
    points, total = vals.shape
    band = gx_size * pad_rows
    pieces = parts.shape[1]

    def turn(pos, step, size):
        if size & (size - 1):
            return lax.rem(pos + step, size) if step else pos
        bit = 1
        while bit <= step:
            if step & bit:
                pos = pos + bit * (1 - 2 * lax.rem(lax.div(pos, bit), 2))
            bit *= 2
        return pos

    def peer(dx, dy, dz):
        return (turn(gx, dx, gx_size), turn(gy, dy, gy_size), turn(gz, dz, gz_size))

    loads = [
        pltpu.make_async_copy(colloc_hbm, vals, load_sem.at[0]),
        pltpu.make_async_copy(core_hbm, core, load_sem.at[1]),
        pltpu.make_async_copy(place_hbm, place, load_sem.at[2]),
        pltpu.make_async_copy(fold_hbm, fold, load_sem.at[3]),
    ]
    spans = [(s, min(DEPTH, total - s)) for s in range(0, total, DEPTH)]
    depth_loads = [
        pltpu.make_async_copy(
            coeffs_hbm.at[pl.ds(s, n)], coeffs.at[pl.ds(s, n)], depth_sem.at[i]
        )
        for i, (s, n) in enumerate(spans)
    ]
    loads[0].start()
    for load in depth_loads:
        load.start()
    loads[1].start()
    loads[2].start()
    loads[3].start()

    barrier = pltpu.get_barrier_semaphore()
    mates = [(dx, 0, dz) for dx in range(gx_size) for dz in range(gz_size) if dx or dz]
    mates += [(0, dy, dz) for dy in range(1, gy_size) for dz in range(gz_size)]
    for mate in mates:
        pl.semaphore_signal(barrier, inc=1, device_id=peer(*mate), device_id_type=MESH)

    sent = []

    def send(src, dst, sems, out_slot, in_slot, target):
        copy = pltpu.make_async_remote_copy(
            src_ref=src,
            dst_ref=dst,
            send_sem=sems.at[(0,) + out_slot],
            recv_sem=sems.at[(1,) + in_slot],
            device_id=target,
            device_id_type=MESH,
        )
        copy.start()
        sent.append(copy)

    def arrive(dst, sems, in_slot, source):
        pltpu.make_async_remote_copy(
            src_ref=dst,
            dst_ref=dst,
            send_sem=sems.at[(0,) + in_slot],
            recv_sem=sems.at[(1,) + in_slot],
            device_id=source,
            device_id_type=MESH,
        ).wait_recv()

    loads[0].wait()
    window = vals.at[:, pl.ds(0, wins.shape[2])]
    occ = jnp.zeros((points, coeffs.shape[1]), F32)
    for load, (s, n) in zip(depth_loads, spans):
        load.wait()
        if s == spans[-1][0]:
            pl.semaphore_wait(barrier, len(mates))
            for dy in range(1, gy_size):
                send(window, wins.at[gy], win_sem, (dy,), (gy,), peer(0, dy, 0))
        occ += dot(vals[:, s : s + n], coeffs[s : s + n, :], 1, 0)
    occ = occ.astype(BF16)
    col_occ[gx] = occ
    row_occ[gy] = occ
    for dy in range(1, gy_size):
        send(row_occ.at[gy], row_occ.at[gy], row_sem, (dy,), (gy,), peer(0, dy, 0))
    for dx in reversed(range(1, gx_size)):
        send(col_occ.at[gx], col_occ.at[gx], col_sem, (dx,), (gx,), peer(dx, 0, 0))

    for load in loads[1:]:
        load.wait()
    own_win = vals[:, : wins.shape[2]]
    wins[gy] = own_win
    spread = place[...]
    win_t[...] = dot(spread, own_win, 0, 1).reshape(gz_size, band, points)
    for a in range(gx_size):
        cores[a] = core[:, a * points : (a + 1) * points]

    def fill(h, c, u, unit):
        at = pl.ds(u * points, points)
        n = min(piece, width - unit * piece)
        s = h * width + unit * piece
        parts[h, c, at, :n] = vals[:, s : s + n]
        if n < piece:
            parts[h, c, at, n:] = jnp.zeros((points, piece - n), BF16)

    for h in range(gy_size):
        for c in range(pieces):
            fill(h, c, 0, c)
            for u in range(tails):
                fill(h, c, 1 + u, pieces + u)

    for dy in range(1, gy_size):
        slot = turn(gy, dy, gy_size)
        arrive(wins.at[slot], win_sem, (slot,), peer(0, dy, 0))
    win_rows = dot(spread, wins[...].reshape(gy_size * points, -1), 0, 1).astype(BF16)
    for dy in range(1, gy_size):
        slot = turn(gy, dy, gy_size)
        arrive(row_occ.at[slot], row_sem, (slot,), peer(0, dy, 0))
    row_vals = row_occ[...].reshape(gy_size * points, -1)

    home = gx * gz_size + gz
    ones = jnp.ones((8, coeffs.shape[1]), BF16)
    potential = jnp.zeros((8, gy_size * points), F32)
    for dx in range(gx_size):
        a = turn(gx, dx, gx_size)
        if dx:
            arrive(col_occ.at[a], col_sem, (a,), peer(dx, 0, 0))
        cols = col_occ[a]
        core_vals = cores[a]
        gram = dot(row_vals, cols, 1, 1)
        mixed = (core_vals.astype(F32) * gram).astype(BF16)
        block = dot(win_rows, mixed, 1, 0).astype(BF16)
        tot_send[a] = block.reshape(gz_size, band, points)
        for dz in range(gz_size):
            if dx or dz:
                to = peer(dx, 0, dz)
                src = tot_send.at[a, to[2]]
                out = (dx * gz_size + dz,)
                send(src, tot_recv.at[home], tot_sem, out, (home,), to)
        square = jnp.square(cols.astype(F32))
        high = square.astype(BF16)
        low = (square - high.astype(F32)).astype(BF16)
        density = dot(ones, high, 1, 1) + dot(ones, low, 1, 1)
        potential += dot(density.astype(BF16), core_vals, 1, 1)
    for h in range(gy_size):
        pot_send[h] = potential[:, h * points : (h + 1) * points]
    mine = gy * gz_size + gz
    for dy in range(gy_size):
        for dz in range(gz_size):
            if dy or dz:
                src = pot_send.at[turn(gy, dy, gy_size)]
                out = (dy * gz_size + dz,)
                send(src, pot_recv.at[mine], pot_sem, out, (mine,), peer(0, dy, dz))

    def spread_out(index, left):
        kept = []
        lefts = [left] * pieces
        if tails:
            folded = dot(fold[...], left, 1, 0).astype(BF16)
            folded = folded.reshape(pieces, tails, band, points)
            lefts = [
                jnp.concatenate([left] + [folded[c, u] for u in range(tails)], axis=1)
                for c in range(pieces)
            ]
        for c in range(pieces):
            for dy in range(1, gy_size):
                h = turn(gy, dy, gy_size)
                y_send[index, c, h] = dot(lefts[c], parts[h, c], 1, 0).astype(BF16)
                slots = (index, c, dy), (index, c, gy)
                dst = y_recv.at[index, c, gy]
                send(y_send.at[index, c, h], dst, y_sem, *slots, peer(0, dy, 0))
        for c in range(pieces):
            kept.append(dot(lefts[c], parts[gy, c], 1, 0))
        return kept

    pot = pot_send[gy]
    for dy in range(gy_size):
        for dz in range(gz_size):
            if dy or dz:
                to = peer(0, dy, dz)
                slot = to[1] * gz_size + to[2]
                arrive(pot_recv.at[slot], pot_sem, (slot,), to)
                pot += pot_recv[slot]
    coul_kept = spread_out(0, (win_t[gz] * pot[:1]).astype(BF16))

    owned = tot_send[gx, gz].astype(F32)
    for dx in range(gx_size):
        for dz in range(gz_size):
            if dx or dz:
                to = peer(dx, 0, dz)
                slot = to[0] * gz_size + to[2]
                arrive(tot_recv.at[slot], tot_sem, (slot,), to)
                owned += tot_recv[slot].astype(F32)
    exch_kept = spread_out(1, owned.astype(BF16))

    for index, kept in enumerate((coul_kept, exch_kept)):
        for c in range(pieces):
            acc = kept[c]
            for dy in range(1, gy_size):
                slot = turn(gy, dy, gy_size)
                dst = y_recv.at[index, c, slot]
                arrive(dst, y_sem, (index, c, slot), peer(0, dy, 0))
                acc += y_recv[index, c, slot].astype(F32)
            z_send[index, c] = acc.reshape(gx_size, pad_rows, piece).astype(BF16)
            for dx in range(1, gx_size):
                a = turn(gx, dx, gx_size)
                slots = (index, c, dx), (index, c, gx)
                dst = z_recv.at[index, c, gx]
                send(z_send.at[index, c, a], dst, z_sem, *slots, peer(dx, 0, 0))

    spare = pad_rows - rows
    for index in range(2):
        for c in range(pieces):
            acc = z_send[index, c, gx].astype(F32)
            for dx in range(1, gx_size):
                slot = turn(gx, dx, gx_size)
                dst = z_recv.at[index, c, slot]
                arrive(dst, z_sem, (index, c, slot), peer(dx, 0, 0))
                acc += z_recv[index, c, slot].astype(F32)
            n = min(piece, width - c * piece)
            out_ref[index, :, c * piece : c * piece + n] = acc[:rows, :n]
            for s in range(spare):
                u, r = divmod(c * spare + s, rows)
                if u < tails:
                    start = (pieces + u) * piece
                    n = min(piece, width - start)
                    line = acc[rows + s : rows + s + 1, :n]
                    out_ref[index, r : r + 1, start : start + n] = line

    for copy in sent:
        copy.wait_send()


def local(colloc, occ_coeffs, core):
    points, total = colloc.shape
    gx_size = lax.axis_size("gx")
    gy_size = lax.axis_size("gy")
    gz_size = lax.axis_size("gz")
    occupied = occ_coeffs.shape[1]
    rows = W // (gx_size * gz_size)
    pad_rows = up(rows, 8)
    width = total // gy_size
    piece = 512 if width > 512 else LANES
    units = -(-width // piece)
    spare = pad_rows - rows
    pieces = next(q for q in range(1, units + 1) if (units - q) * rows <= q * spare)
    tails = units - pieces
    row_count, flat = core.shape[0], core.shape[2]
    band = gx_size * pad_rows
    lanes = up(W, LANES)

    place = np.zeros((lanes, gz_size, gx_size, pad_rows), np.float32)
    for a in range(gx_size):
        for g in range(gz_size):
            for k in range(rows):
                place[(a * gz_size + g) * rows + k, g, a, k] = 1
    place = jnp.asarray(place.reshape(lanes, gz_size * band), BF16)

    fold = np.zeros((pieces, max(tails, 1), band, band), np.float32)
    for c in range(pieces):
        for s in range(spare):
            u, r = divmod(c * spare + s, rows)
            if u < tails:
                for a in range(0, band, pad_rows):
                    fold[c, u, a + rows + s, a + r] = 1
    fold = jnp.asarray(fold.reshape(-1, band), BF16)

    dims = (gx_size, gy_size, gz_size, rows, pad_rows, width, piece, tails)
    dma = pltpu.SemaphoreType.DMA
    vmem = pltpu.VMEM
    result = pl.pallas_call(
        functools.partial(kernel, dims),
        out_shape=jax.ShapeDtypeStruct((2, rows, width), F32),
        in_specs=[pl.BlockSpec(memory_space=pltpu.HBM)] * 5,
        out_specs=pl.BlockSpec(memory_space=pltpu.VMEM),
        scratch_shapes=[
            vmem((points, total), BF16),
            vmem((total, occupied), BF16),
            vmem((row_count, flat), BF16),
            vmem((lanes, gz_size * band), BF16),
            vmem(fold.shape, BF16),
            vmem((gx_size, row_count, points), BF16),
            vmem((gx_size, points, occupied), BF16),
            vmem((gy_size, points, occupied), BF16),
            vmem((gy_size, points, lanes), BF16),
            vmem((gz_size, band, points), F32),
            vmem((gy_size, pieces, (1 + tails) * points, piece), BF16),
            vmem((gy_size, 8, points), F32),
            vmem((gy_size * gz_size, 8, points), F32),
            vmem((gx_size, gz_size, band, points), BF16),
            vmem((gx_size * gz_size, band, points), BF16),
            vmem((2, pieces, gy_size, band, piece), BF16),
            vmem((2, pieces, gy_size, band, piece), BF16),
            vmem((2, pieces, gx_size, pad_rows, piece), BF16),
            vmem((2, pieces, gx_size, pad_rows, piece), BF16),
            dma((4,)),
            dma((-(-total // DEPTH),)),
            dma((2, gx_size)),
            dma((2, gy_size)),
            dma((2, gy_size)),
            dma((2, gy_size * gz_size)),
            dma((2, gx_size * gz_size)),
            dma((2, 2, pieces, gy_size)),
            dma((2, 2, pieces, gx_size)),
        ],
        compiler_params=pltpu.CompilerParams(
            collective_id=0, has_side_effects=True, vmem_limit_bytes=67043328
        ),
    )(colloc, occ_coeffs, core.reshape(row_count, flat), place, fold)
    return result[0], result[1]


def solution(mesh):
    in_specs = (P(("gx", "gy"), None), P(None, "gz"), P("gx", "gy", None))
    out_specs = (P(("gx", "gz"), "gy"), P(("gx", "gz"), "gy"))
    return jax.shard_map(local, mesh=mesh, in_specs=in_specs, out_specs=out_specs, check_vma=False)
```

```python
import functools

import jax
import jax.numpy as jnp
import numpy as np
from jax import lax
from jax.experimental import pallas as pl
from jax.experimental.pallas import tpu as pltpu
from jax.sharding import PartitionSpec as P

W = 96
LANES = 128
DEPTH = 1024
MESH = pl.DeviceIdType.MESH
F32 = jnp.float32
BF16 = jnp.bfloat16


def up(value, step):
    return -(-value // step) * step


def dot(left, right, left_dim, right_dim):
    return lax.dot_general(
        left, right, (((left_dim,), (right_dim,)), ((), ())), preferred_element_type=F32
    )


def kernel(
    dims,
    colloc_hbm,
    coeffs_hbm,
    core_hbm,
    place_hbm,
    fold_hbm,
    out_ref,
    vals,
    coeffs,
    core,
    place,
    fold,
    cores,
    col_occ,
    row_occ,
    wins,
    win_t,
    parts,
    pot_send,
    pot_recv,
    tot_send,
    tot_recv,
    y_send,
    y_recv,
    z_send,
    z_recv,
    load_sem,
    depth_sem,
    col_sem,
    row_sem,
    win_sem,
    pot_sem,
    tot_sem,
    y_sem,
    z_sem,
):
    gx_size, gy_size, gz_size, rows, pad_rows, width, piece, tails = dims
    gx, gy, gz = lax.axis_index("gx"), lax.axis_index("gy"), lax.axis_index("gz")
    points, total = vals.shape
    band = gx_size * pad_rows
    pieces = parts.shape[1]
    slabs, _, slab = coeffs.shape

    def turn(pos, step, size):
        if size & (size - 1):
            return lax.rem(pos + step, size) if step else pos
        bit = 1
        while bit <= step:
            if step & bit:
                pos = pos + bit * (1 - 2 * lax.rem(lax.div(pos, bit), 2))
            bit *= 2
        return pos

    def peer(dx, dy, dz):
        return (turn(gx, dx, gx_size), turn(gy, dy, gy_size), turn(gz, dz, gz_size))

    loads = [
        pltpu.make_async_copy(colloc_hbm, vals, load_sem.at[0]),
        pltpu.make_async_copy(core_hbm, core, load_sem.at[1]),
        pltpu.make_async_copy(place_hbm, place, load_sem.at[2]),
        pltpu.make_async_copy(fold_hbm, fold, load_sem.at[3]),
    ]
    spans = [(s, min(DEPTH, total - s)) for s in range(0, total, DEPTH)]
    depth_loads = [
        pltpu.make_async_copy(
            coeffs_hbm.at[pl.ds(s, n), pl.ds(q * slab, slab)],
            coeffs.at[q, pl.ds(s, n)],
            depth_sem.at[q, i],
        )
        for q in range(slabs)
        for i, (s, n) in enumerate(spans)
    ]
    loads[0].start()
    for load in depth_loads:
        load.start()
    loads[1].start()
    loads[2].start()
    loads[3].start()

    barrier = pltpu.get_barrier_semaphore()
    mates = [(dx, 0, dz) for dx in range(gx_size) for dz in range(gz_size) if dx or dz]
    mates += [(0, dy, dz) for dy in range(1, gy_size) for dz in range(gz_size)]
    for mate in mates:
        pl.semaphore_signal(barrier, inc=1, device_id=peer(*mate), device_id_type=MESH)

    sent = []

    def send(src, dst, sems, out_slot, in_slot, target):
        copy = pltpu.make_async_remote_copy(
            src_ref=src,
            dst_ref=dst,
            send_sem=sems.at[(0,) + out_slot],
            recv_sem=sems.at[(1,) + in_slot],
            device_id=target,
            device_id_type=MESH,
        )
        copy.start()
        sent.append(copy)

    def arrive(dst, sems, in_slot, source):
        pltpu.make_async_remote_copy(
            src_ref=dst,
            dst_ref=dst,
            send_sem=sems.at[(0,) + in_slot],
            recv_sem=sems.at[(1,) + in_slot],
            device_id=source,
            device_id_type=MESH,
        ).wait_recv()

    loads[0].wait()
    window = vals.at[:, pl.ds(0, wins.shape[2])]
    for q in range(slabs):
        occ = jnp.zeros((points, slab), F32)
        for i, (s, n) in enumerate(spans):
            depth_loads[q * len(spans) + i].wait()
            occ += dot(vals[:, s : s + n], coeffs[q, s : s + n, :], 1, 0)
        occ = occ.astype(BF16)
        col_occ[gx, q] = occ
        row_occ[gy, q] = occ
        if q == 0:
            pl.semaphore_wait(barrier, len(mates))
        for dx in reversed(range(1, gx_size)):
            slots = (dx, q), (gx, q)
            src = col_occ.at[gx, q]
            send(src, src, col_sem, *slots, peer(dx, 0, 0))
        for dy in range(1, gy_size):
            slots = (dy, q), (gy, q)
            src = row_occ.at[gy, q]
            send(src, src, row_sem, *slots, peer(0, dy, 0))
        if q == 0:
            for dy in range(1, gy_size):
                send(window, wins.at[gy], win_sem, (dy,), (gy,), peer(0, dy, 0))

    for load in loads[1:]:
        load.wait()
    own_win = vals[:, : wins.shape[2]]
    wins[gy] = own_win
    spread = place[...]
    win_t[...] = dot(spread, own_win, 0, 1).reshape(gz_size, band, points)
    for a in range(gx_size):
        cores[a] = core[:, a * points : (a + 1) * points]

    def fill(h, c, u, unit):
        at = pl.ds(u * points, points)
        n = min(piece, width - unit * piece)
        s = h * width + unit * piece
        parts[h, c, at, :n] = vals[:, s : s + n]
        if n < piece:
            parts[h, c, at, n:] = jnp.zeros((points, piece - n), BF16)

    for h in range(gy_size):
        for c in range(pieces):
            fill(h, c, 0, c)
            for u in range(tails):
                fill(h, c, 1 + u, pieces + u)

    for dy in range(1, gy_size):
        slot = turn(gy, dy, gy_size)
        arrive(wins.at[slot], win_sem, (slot,), peer(0, dy, 0))
    win_rows = dot(spread, wins[...].reshape(gy_size * points, -1), 0, 1).astype(BF16)
    for dy in range(1, gy_size):
        slot = turn(gy, dy, gy_size)
        for q in range(slabs):
            arrive(row_occ.at[slot, q], row_sem, (slot, q), peer(0, dy, 0))
    row_vals = [row_occ[:, q].reshape(gy_size * points, slab) for q in range(slabs)]
    row_vals = jnp.concatenate(row_vals, axis=1)

    home = gx * gz_size + gz
    ones = jnp.ones((8, slabs * slab), BF16)
    potential = jnp.zeros((8, gy_size * points), F32)
    for dx in range(gx_size):
        a = turn(gx, dx, gx_size)
        if dx:
            for q in range(slabs):
                arrive(col_occ.at[a, q], col_sem, (a, q), peer(dx, 0, 0))
        cols = jnp.concatenate([col_occ[a, q] for q in range(slabs)], axis=1)
        core_vals = cores[a]
        gram = dot(row_vals, cols, 1, 1)
        mixed = (core_vals.astype(F32) * gram).astype(BF16)
        block = dot(win_rows, mixed, 1, 0).astype(BF16)
        tot_send[a] = block.reshape(gz_size, band, points)
        for dz in range(gz_size):
            if dx or dz:
                to = peer(dx, 0, dz)
                src = tot_send.at[a, to[2]]
                out = (dx * gz_size + dz,)
                send(src, tot_recv.at[home], tot_sem, out, (home,), to)
        square = jnp.square(cols.astype(F32))
        high = square.astype(BF16)
        low = (square - high.astype(F32)).astype(BF16)
        density = dot(ones, high, 1, 1) + dot(ones, low, 1, 1)
        potential += dot(density.astype(BF16), core_vals, 1, 1)
    for h in range(gy_size):
        pot_send[h] = potential[:, h * points : (h + 1) * points]
    mine = gy * gz_size + gz
    for dy in range(gy_size):
        for dz in range(gz_size):
            if dy or dz:
                src = pot_send.at[turn(gy, dy, gy_size)]
                out = (dy * gz_size + dz,)
                send(src, pot_recv.at[mine], pot_sem, out, (mine,), peer(0, dy, dz))

    def spread_out(index, left):
        kept = []
        lefts = [left] * pieces
        if tails:
            folded = dot(fold[...], left, 1, 0).astype(BF16)
            folded = folded.reshape(pieces, tails, band, points)
            lefts = [
                jnp.concatenate([left] + [folded[c, u] for u in range(tails)], axis=1)
                for c in range(pieces)
            ]
        for c in range(pieces):
            for dy in range(1, gy_size):
                h = turn(gy, dy, gy_size)
                y_send[index, c, h] = dot(lefts[c], parts[h, c], 1, 0).astype(BF16)
                slots = (index, c, dy), (index, c, gy)
                dst = y_recv.at[index, c, gy]
                send(y_send.at[index, c, h], dst, y_sem, *slots, peer(0, dy, 0))
        for c in range(pieces):
            kept.append(dot(lefts[c], parts[gy, c], 1, 0))
        return kept

    pot = pot_send[gy]
    for dy in range(gy_size):
        for dz in range(gz_size):
            if dy or dz:
                to = peer(0, dy, dz)
                slot = to[1] * gz_size + to[2]
                arrive(pot_recv.at[slot], pot_sem, (slot,), to)
                pot += pot_recv[slot]
    coul_kept = spread_out(0, (win_t[gz] * pot[:1]).astype(BF16))

    owned = tot_send[gx, gz].astype(F32)
    for dx in range(gx_size):
        for dz in range(gz_size):
            if dx or dz:
                to = peer(dx, 0, dz)
                slot = to[0] * gz_size + to[2]
                arrive(tot_recv.at[slot], tot_sem, (slot,), to)
                owned += tot_recv[slot].astype(F32)
    exch_kept = spread_out(1, owned.astype(BF16))

    for index, kept in enumerate((coul_kept, exch_kept)):
        for c in range(pieces):
            acc = kept[c]
            for dy in range(1, gy_size):
                slot = turn(gy, dy, gy_size)
                dst = y_recv.at[index, c, slot]
                arrive(dst, y_sem, (index, c, slot), peer(0, dy, 0))
                acc += y_recv[index, c, slot].astype(F32)
            z_send[index, c] = acc.reshape(gx_size, pad_rows, piece).astype(BF16)
            for dx in range(1, gx_size):
                a = turn(gx, dx, gx_size)
                slots = (index, c, dx), (index, c, gx)
                dst = z_recv.at[index, c, gx]
                send(z_send.at[index, c, a], dst, z_sem, *slots, peer(dx, 0, 0))

    spare = pad_rows - rows
    for index in range(2):
        for c in range(pieces):
            acc = z_send[index, c, gx].astype(F32)
            for dx in range(1, gx_size):
                slot = turn(gx, dx, gx_size)
                dst = z_recv.at[index, c, slot]
                arrive(dst, z_sem, (index, c, slot), peer(dx, 0, 0))
                acc += z_recv[index, c, slot].astype(F32)
            n = min(piece, width - c * piece)
            out_ref[index, :, c * piece : c * piece + n] = acc[:rows, :n]
            for s in range(spare):
                u, r = divmod(c * spare + s, rows)
                if u < tails:
                    start = (pieces + u) * piece
                    n = min(piece, width - start)
                    line = acc[rows + s : rows + s + 1, :n]
                    out_ref[index, r : r + 1, start : start + n] = line

    for copy in sent:
        copy.wait_send()


def local(colloc, occ_coeffs, core):
    points, total = colloc.shape
    gx_size = lax.axis_size("gx")
    gy_size = lax.axis_size("gy")
    gz_size = lax.axis_size("gz")
    occupied = occ_coeffs.shape[1]
    rows = W // (gx_size * gz_size)
    pad_rows = up(rows, 8)
    width = total // gy_size
    piece = 512 if width > 512 else LANES
    units = -(-width // piece)
    spare = pad_rows - rows
    pieces = next(q for q in range(1, units + 1) if (units - q) * rows <= q * spare)
    tails = units - pieces
    row_count, flat = core.shape[0], core.shape[2]
    slab = LANES if occupied % LANES == 0 else occupied
    slabs = occupied // slab
    band = gx_size * pad_rows
    lanes = up(W, LANES)

    place = np.zeros((lanes, gz_size, gx_size, pad_rows), np.float32)
    for a in range(gx_size):
        for g in range(gz_size):
            for k in range(rows):
                place[(a * gz_size + g) * rows + k, g, a, k] = 1
    place = jnp.asarray(place.reshape(lanes, gz_size * band), BF16)

    fold = np.zeros((pieces, max(tails, 1), band, band), np.float32)
    for c in range(pieces):
        for s in range(spare):
            u, r = divmod(c * spare + s, rows)
            if u < tails:
                for a in range(0, band, pad_rows):
                    fold[c, u, a + rows + s, a + r] = 1
    fold = jnp.asarray(fold.reshape(-1, band), BF16)

    dims = (gx_size, gy_size, gz_size, rows, pad_rows, width, piece, tails)
    dma = pltpu.SemaphoreType.DMA
    vmem = pltpu.VMEM
    result = pl.pallas_call(
        functools.partial(kernel, dims),
        out_shape=pltpu.VMEM((2, rows, width), F32),
        in_specs=[pl.BlockSpec(memory_space=pltpu.HBM)] * 5,
        out_specs=pl.BlockSpec(memory_space=pltpu.VMEM),
        scratch_shapes=[
            vmem((points, total), BF16),
            vmem((slabs, total, slab), BF16),
            vmem((row_count, flat), BF16),
            vmem((lanes, gz_size * band), BF16),
            vmem(fold.shape, BF16),
            vmem((gx_size, row_count, points), BF16),
            vmem((gx_size, slabs, points, slab), BF16),
            vmem((gy_size, slabs, points, slab), BF16),
            vmem((gy_size, points, lanes), BF16),
            vmem((gz_size, band, points), F32),
            vmem((gy_size, pieces, (1 + tails) * points, piece), BF16),
            vmem((gy_size, 8, points), F32),
            vmem((gy_size * gz_size, 8, points), F32),
            vmem((gx_size, gz_size, band, points), BF16),
            vmem((gx_size * gz_size, band, points), BF16),
            vmem((2, pieces, gy_size, band, piece), BF16),
            vmem((2, pieces, gy_size, band, piece), BF16),
            vmem((2, pieces, gx_size, pad_rows, piece), BF16),
            vmem((2, pieces, gx_size, pad_rows, piece), BF16),
            dma((4,)),
            dma((slabs, -(-total // DEPTH))),
            dma((2, gx_size, slabs)),
            dma((2, gy_size, slabs)),
            dma((2, gy_size)),
            dma((2, gy_size * gz_size)),
            dma((2, gx_size * gz_size)),
            dma((2, 2, pieces, gy_size)),
            dma((2, 2, pieces, gx_size)),
        ],
        compiler_params=pltpu.CompilerParams(
            collective_id=0, has_side_effects=True, vmem_limit_bytes=60 * 1024 * 1024
        ),
    )(colloc, occ_coeffs, core.reshape(row_count, flat), place, fold)
    return result[0], result[1]


def solution(mesh):
    in_specs = (P(("gx", "gy"), None), P(None, "gz"), P("gx", "gy", None))
    out_specs = (P(("gx", "gz"), "gy"), P(("gx", "gz"), "gy"))
    return jax.shard_map(local, mesh=mesh, in_specs=in_specs, out_specs=out_specs, check_vma=False)
```
